8 devices in a mesh: dp: 1 (over z), tp2: 2 (over y), tp: 4 (over x, core).
Axes of the slice: x: 2, y: 2, z: 1, core: 2. Of those that a mesh axis runs over, the one named last changes fastest.
Arguments:
- attn_out: bfloat16 [4096, 16384], P('dp', 'tp')
- w_out: bfloat16 [16384, 16384], P('tp', 'tp2')
- residual: bfloat16 [4096, 16384], P(('dp', 'tp'), 'tp2')
- norm_gain: float32 [16384], P('tp2')
Outputs:
- output 1: bfloat16 [4096, 16384], P(('dp', 'tp'), 'tp2')
- output 2: bfloat16 [4096, 16384], P(('dp', 'tp'), 'tp2')
All inputs are finite; a program needn't handle non-finite values.
Results may differ from the reference program's by a relative error of at most 0.00721035.
Values are sent between devices in bfloat16 or wider.
A program may use at most 1 GiB of HBM per device.

```python
import jax
import jax.numpy as jnp
from jax import lax

TOKENS = 4096
D = 16384
HEADS = 128
HEAD = 128
TP = 4
EPS_NORM = 1e-6


def setup_inputs(seed: int = 0, part: int = 0) -> dict:
    attn_width = HEADS * HEAD
    root_key = jax.random.key(seed)
    key_attn, key_w, key_res, key_gain = jax.random.split(root_key, 4)
    attn_vals = jax.random.normal(jax.random.fold_in(key_attn, part), (TOKENS, attn_width), jnp.float32)
    w_vals = jax.random.normal(key_w, (attn_width, D), jnp.float32) * (attn_width ** -0.5)
    res_vals = jax.random.normal(jax.random.fold_in(key_res, part), (TOKENS, D), jnp.float32)
    gain_vals = 1.0 + 0.3 * jax.random.normal(key_gain, (D,), jnp.float32)
    return {"attn_out": attn_vals.astype(jnp.bfloat16), "w_out": w_vals.astype(jnp.bfloat16), "residual": res_vals.astype(jnp.bfloat16), "norm_gain": gain_vals}


def reference(attn_out, w_out, residual, norm_gain):
    attn_width = attn_out.shape[1]
    shard_cols = attn_width // TP
    attn_shards = attn_out.reshape(TOKENS, TP, shard_cols).transpose(1, 0, 2)
    w_shards = w_out.reshape(TP, shard_cols, D)

    def add_shard(running, shard_pair):
        attn_blk, w_blk = shard_pair
        block_prod = jnp.dot(attn_blk, w_blk, preferred_element_type=jnp.float32).astype(jnp.bfloat16)
        return running + block_prod.astype(jnp.float32), None

    y_sum, _ = lax.scan(add_shard, jnp.zeros((TOKENS, D), jnp.float32), (attn_shards, w_shards))
    hidden = residual.astype(jnp.float32) + y_sum
    mean_sq = jnp.mean(hidden * hidden, axis=-1, keepdims=True)
    normed = hidden * lax.rsqrt(mean_sq + EPS_NORM) * norm_gain
    return hidden.astype(jnp.bfloat16), normed.astype(jnp.bfloat16)
```

```python
import jax
import jax.numpy as jnp
from jax import lax
from jax.experimental import pallas as pl
from jax.experimental.pallas import tpu as pltpu
from jax.sharding import PartitionSpec as P


EPS_NORM = 1e-6
F32, BF16 = jnp.float32, jnp.bfloat16
VMEM_BYTES = 67043328

ANY = pl.BlockSpec(memory_space=pl.ANY)
PARAMS = pltpu.CompilerParams(vmem_limit_bytes=VMEM_BYTES)


def products(attn, w, blocks, reps, tm, col0, ncols, tn, splits, deps):
    depth = attn.shape[1]
    nb, ns = len(blocks), len(splits)
    index = jnp.stack(blocks).astype(jnp.int32)

    def body(index_ref, *refs):
        a_refs, w_ref = refs[:nb], refs[nb]
        outs = refs[nb + 1 + len(deps):]
        for b in range(nb):
            val = jnp.dot(a_refs[b][...], w_ref[...], preferred_element_type=F32).astype(BF16)
            row = 0
            for s, size in enumerate(splits):
                outs[b * ns + s][...] = val[row:row + size]
                row += size

    c0 = col0 // tn
    a_specs = [pl.BlockSpec((tm, depth), lambda j, i, idx, b=b: (idx[b] + i, 0)) for b in range(nb)]
    w_spec = pl.BlockSpec((depth, tn), lambda j, i, idx: (0, c0 + j))
    out_specs = [pl.BlockSpec((size, tn), lambda j, i, idx: (i, j)) for _ in range(nb) for size in splits]
    return pl.pallas_call(
        body,
        grid_spec=pltpu.PrefetchScalarGridSpec(
            num_scalar_prefetch=1,
            grid=(ncols // tn, reps),
            in_specs=a_specs + [w_spec] + [ANY] * len(deps),
            out_specs=out_specs,
        ),
        out_shape=[jax.ShapeDtypeStruct((size * reps, ncols), BF16) for _ in range(nb) for size in splits],
        compiler_params=PARAMS,
        cost_estimate=pl.CostEstimate(
            flops=2 * nb * reps * tm * depth * ncols,
            bytes_accessed=2 * (depth * ncols + nb * reps * tm * (depth + ncols)),
            transcendentals=0),
    )(index, *([attn] * nb), w, *deps)


def add_rows(res, near, far, row0, rows, tr, state, deps):
    total_rows, cols = res.shape
    nn, nf, per = len(near), len(far), len(far[0])
    widths = [piece.shape[1] for piece in far[0]]
    flat = [piece for group in far for piece in group]

    def body(*refs):
        r_ref, near_refs, far_refs = refs[0], refs[1:1 + nn], refs[1 + nn:1 + nn + nf * per]
        h_ref, ho_ref, sq_ref = refs[-3:]
        total = jnp.zeros((tr, 1), F32)
        base = 0
        for c, width in enumerate(widths):
            sl = slice(base, base + width)
            y = near_refs[0][:, sl].astype(F32)
            for ref in near_refs[1:]:
                y = y + ref[:, sl].astype(F32)
            for g in range(nf):
                y = y + far_refs[g * per + c][...].astype(F32)
            h = r_ref[:, sl].astype(F32) + y
            h_ref[:, sl] = h
            ho_ref[:, sl] = h.astype(BF16)
            total = total + jnp.sum(h * h, axis=-1, keepdims=True)
            base += width
        sq_ref[...] = total

    b0 = row0 // tr
    full = pl.BlockSpec((tr, cols), lambda i: (b0 + i, 0))
    in_specs = [full] * (1 + nn) + [pl.BlockSpec((tr, piece.shape[1]), lambda i: (i, 0)) for piece in flat]
    args = [res, *near, *flat]
    in_specs += [ANY] * (len(deps) + len(state))
    args += [*deps, *state]
    first = len(args) - len(state)
    return pl.pallas_call(
        body,
        grid=(rows // tr,),
        in_specs=in_specs,
        out_specs=[full, full, pl.BlockSpec((tr, 1), lambda i: (b0 + i, 0))],
        out_shape=[
            jax.ShapeDtypeStruct((total_rows, cols), F32),
            jax.ShapeDtypeStruct((total_rows, cols), BF16),
            jax.ShapeDtypeStruct((total_rows, 1), F32),
        ],
        input_output_aliases={first + i: i for i in range(len(state))},
        compiler_params=PARAMS,
        cost_estimate=pl.CostEstimate(flops=8 * rows * cols, bytes_accessed=16 * rows * cols, transcendentals=0),
    )(*args)


def norm_rows(h, sq, gain, width, row0, rows, sq_row0, tr, n_out):
    total_rows, cols = h.shape

    def body(*refs):
        h_ref, sq_ref, g_ref, n_ref = refs[0], refs[1], refs[2], refs[-1]
        inv = lax.rsqrt(sq_ref[...] / width + EPS_NORM)
        n_ref[...] = (h_ref[...] * inv * g_ref[...]).astype(BF16)

    b0, s0 = row0 // tr, sq_row0 // tr
    in_specs = [
        pl.BlockSpec((tr, cols), lambda i: (b0 + i, 0)),
        pl.BlockSpec((tr, 1), lambda i: (s0 + i, 0)),
        pl.BlockSpec((1, cols), lambda i: (0, 0)),
    ]
    args = [h, sq, gain]
    if n_out is not None:
        in_specs.append(ANY)
        args.append(n_out)
    return pl.pallas_call(
        body,
        grid=(rows // tr,),
        in_specs=in_specs,
        out_specs=pl.BlockSpec((tr, cols), lambda i: (b0 + i, 0)),
        out_shape=jax.ShapeDtypeStruct((total_rows, cols), BF16),
        input_output_aliases={} if n_out is None else {3: 0},
        compiler_params=PARAMS,
        cost_estimate=pl.CostEstimate(flops=4 * rows * cols, bytes_accessed=6 * rows * cols, transcendentals=0),
    )(*args)


TM = 256
FIRST_COLS = (512, 1536, 6144)
LAST_ROWS = (128, 64, 64)


def solution(mesh):
    tp = mesh.shape["tp"]
    col_groups = mesh.shape["tp2"]

    def send(x, flip):
        return lax.ppermute(x, "tp", [(i, i ^ flip) for i in range(tp)])

    def inner(attn, w, res, gain):
        me = lax.axis_index("tp")
        rows_total, cols = res.shape
        per = rows_total // TM
        plan, col0 = [], 0
        for ncols in FIRST_COLS:
            plan.append((0, col0, ncols, 512, (TM,)))
            col0 += ncols
        plan += [(k, 0, cols, 512, (TM,)) for k in range(1, per - 1)]
        plan += [(per - 1, 0, cols, 512, LAST_ROWS)]
        near_at = len(FIRST_COLS) + 1
        pieces = {}
        dep = []
        near = None

        for t, (k, col0, ncols, tn, splits) in enumerate(plan):
            if t == near_at:
                other, own = products(attn, w, [(me ^ 1) * per, me * per], per, TM, 0, cols, 1024, (TM,), dep)
                dep = [own]
                near = [own, send(other, 1)]
            outs = products(attn, w, [(me ^ 2) * per + k, (me ^ 3) * per + k], 1, TM, col0, ncols, tn, splits, dep)
            dep = [outs[0]]
            row = k * TM
            for s, size in enumerate(splits):
                got = pieces.setdefault((row, size), ([], []))
                for b, flip in enumerate((2, 3)):
                    got[b].append(send(outs[b * len(splits) + s], flip))
                row += size

        chunks = sorted(pieces)
        gain2 = gain.reshape(1, cols)
        state = []
        for c, (row, size) in enumerate(chunks[:-1]):
            state = add_rows(res, near, pieces[row, size], row, size, 64, state, dep if c == 0 else [])
        last, last_size = chunks[-1]
        h, h_out, sq = state
        sq_a = lax.psum(sq, "tp2")
        n_out = norm_rows(h, sq_a, gain2, cols * col_groups, 0, last, 0, 64, None)
        h, h_out, sq = add_rows(res, near, pieces[last, last_size], last, last_size, last_size, state, [n_out])
        sq_b = lax.psum(sq[last:], "tp2")
        n_out = norm_rows(h, sq_b, gain2, cols * col_groups, last, last_size, 0, last_size, n_out)
        return h_out, n_out

    row_spec = P(("dp", "tp"), "tp2")
    fn = jax.shard_map(inner, mesh=mesh, in_specs=(P("dp", "tp"), P("tp", "tp2"), row_spec, P("tp2")), out_specs=(row_spec, row_spec), check_vma=False)
    shapes = [jax.ShapeDtypeStruct(s, d) for s, d in (((4096, 16384), BF16), ((16384, 16384), BF16), ((4096, 16384), BF16), ((16384,), F32))]
    jax.eval_shape(fn, *shapes)
    return fn
```

```python
import jax
import jax.numpy as jnp
from jax import lax
from jax.experimental import pallas as pl
from jax.experimental.pallas import tpu as pltpu
from jax.sharding import PartitionSpec as P


EPS_NORM = 1e-6
F32, BF16 = jnp.float32, jnp.bfloat16
VMEM_BYTES = 67043328

ANY = pl.BlockSpec(memory_space=pl.ANY)
PARAMS = pltpu.CompilerParams(vmem_limit_bytes=VMEM_BYTES)

PLAN = (
    (0, 128, 0, 512, 256, (128,)),
    (0, 128, 512, 1024, 256, (128,)),
    (0, 128, 1536, 2560, 512, (128,)),
    (0, 128, 4096, 4096, 512, (128,)),
    (128, 128, 0, 8192, 512, (128,)),
    (256, 256, 0, 8192, 512, (256,)),
    (512, 256, 0, 8192, 512, (256,)),
    (768, 256, 0, 8192, 512, (128, 96, 32)),
)
NEAR_AT = 6
NEAR_ROWS = 256


def products(attn, w, blocks, reps, tm, col0, ncols, tn, splits, deps):
    depth = attn.shape[1]
    nb, ns = len(blocks), len(splits)

    def body(*refs):
        a_refs, w_ref = refs[nb:2 * nb], refs[2 * nb]
        outs = refs[2 * nb + 1 + len(deps):]
        for b in range(nb):
            val = jnp.dot(a_refs[b][...], w_ref[...], preferred_element_type=F32).astype(BF16)
            row = 0
            for s, size in enumerate(splits):
                outs[b * ns + s][...] = val[row:row + size]
                row += size

    c0 = col0 // tn
    a_specs = [pl.BlockSpec((tm, depth), lambda j, i, *idx, b=b: (idx[b][0] + i, 0)) for b in range(nb)]
    w_spec = pl.BlockSpec((depth, tn), lambda j, i, *idx: (0, c0 + j))
    out_specs = [pl.BlockSpec((size, tn), lambda j, i, *idx: (i, j)) for _ in range(nb) for size in splits]
    return pl.pallas_call(
        body,
        grid_spec=pltpu.PrefetchScalarGridSpec(
            num_scalar_prefetch=nb,
            grid=(ncols // tn, reps),
            in_specs=a_specs + [w_spec] + [ANY] * len(deps),
            out_specs=out_specs,
        ),
        out_shape=[jax.ShapeDtypeStruct((size * reps, ncols), BF16) for _ in range(nb) for size in splits],
        compiler_params=PARAMS,
        cost_estimate=pl.CostEstimate(
            flops=2 * nb * reps * tm * depth * ncols,
            bytes_accessed=2 * (depth * ncols + nb * reps * tm * (depth + ncols)),
            transcendentals=0),
    )(*[b.reshape(1).astype(jnp.int32) for b in blocks], *([attn] * nb), w, *deps)


def add_rows(res, near, far, row0, rows, tr, peers, deps, collective_id):
    cols = res.shape[1]
    nn, nf, per = len(near), len(far), len(far[0])
    widths = [piece.shape[1] for piece in far[0]]
    flat = [piece for group in far for piece in group]
    steps = rows // tr

    def body(*refs):
        r_ref, near_refs, far_refs = refs[0], refs[1:1 + nn], refs[1 + nn:1 + nn + nf * per]
        h_ref, sq_ref, mine, theirs, send_sem, recv_sem = refs[-6:]
        i = pl.program_id(0)
        peer = {"tp2": peers - 1 - lax.axis_index("tp2")}
        barrier = pltpu.get_barrier_semaphore()

        @pl.when(i == 0)
        def _():
            pl.semaphore_signal(barrier, inc=1, device_id=peer, device_id_type=pl.DeviceIdType.MESH)

        total = jnp.zeros((tr, 1), F32)
        base = 0
        for c, width in enumerate(widths):
            sl = slice(base, base + width)
            y = near_refs[0][:, sl].astype(F32)
            for ref in near_refs[1:]:
                y = y + ref[:, sl].astype(F32)
            for g in range(nf):
                y = y + far_refs[g * per + c][...].astype(F32)
            h = r_ref[:, sl].astype(F32) + y
            h_ref[:, sl] = h
            total = total + jnp.sum(h * h, axis=-1, keepdims=True)
            base += width
        mine[pl.ds(pl.multiple_of(i * tr, tr), tr), :] = jnp.broadcast_to(total, (tr, 128))

        @pl.when(i == steps - 1)
        def _():
            pl.semaphore_wait(barrier, 1)
            copy = pltpu.make_async_remote_copy(
                src_ref=mine, dst_ref=theirs, send_sem=send_sem, recv_sem=recv_sem,
                device_id=peer, device_id_type=pl.DeviceIdType.MESH)
            copy.start()
            copy.wait()
            sq_ref[...] = mine[...] + theirs[...]

    b0 = row0 // tr
    full = pl.BlockSpec((tr, cols), lambda i: (b0 + i, 0))
    in_specs = [full] * (1 + nn) + [pl.BlockSpec((tr, piece.shape[1]), lambda i: (i, 0)) for piece in flat] + [ANY] * len(deps)
    return pl.pallas_call(
        body,
        grid=(steps,),
        in_specs=in_specs,
        out_specs=[pl.BlockSpec((tr, cols), lambda i: (i, 0)), pl.BlockSpec((rows, 128), lambda i: (0, 0))],
        out_shape=[jax.ShapeDtypeStruct((rows, cols), F32), jax.ShapeDtypeStruct((rows, 128), F32)],
        scratch_shapes=[
            pltpu.VMEM((rows, 128), F32),
            pltpu.VMEM((rows, 128), F32),
            pltpu.SemaphoreType.DMA,
            pltpu.SemaphoreType.DMA,
        ],
        compiler_params=pltpu.CompilerParams(vmem_limit_bytes=VMEM_BYTES, collective_id=collective_id, has_side_effects=True),
        cost_estimate=pl.CostEstimate(flops=8 * rows * cols, bytes_accessed=14 * rows * cols, transcendentals=0),
    )(res, *near, *flat, *deps)


def norm_rows(h, sq, gain, width, total_rows, row0, tr, state):
    rows, cols = h.shape

    def body(*refs):
        h_ref, sq_ref, g_ref, ho_ref, n_ref = refs[0], refs[1], refs[2], refs[-2], refs[-1]
        inv = lax.rsqrt(sq_ref[:, :1] / width + EPS_NORM)
        h = h_ref[...]
        ho_ref[...] = h.astype(BF16)
        n_ref[...] = (h * inv * g_ref[...]).astype(BF16)

    b0 = row0 // tr
    in_specs = [
        pl.BlockSpec((tr, cols), lambda i: (i, 0)),
        pl.BlockSpec((tr, 128), lambda i: (i, 0)),
        pl.BlockSpec((1, cols), lambda i: (0, 0)),
    ] + [ANY] * len(state)
    out = jax.ShapeDtypeStruct((total_rows, cols), BF16)
    return pl.pallas_call(
        body,
        grid=(rows // tr,),
        in_specs=in_specs,
        out_specs=[pl.BlockSpec((tr, cols), lambda i: (b0 + i, 0))] * 2,
        out_shape=[out, out],
        input_output_aliases={3 + i: i for i in range(len(state))},
        compiler_params=PARAMS,
        cost_estimate=pl.CostEstimate(flops=4 * rows * cols, bytes_accessed=8 * rows * cols, transcendentals=0),
    )(h, sq, gain, *state)


def solution(mesh):
    tp = mesh.shape["tp"]
    col_groups = mesh.shape["tp2"]

    def send(x, flip):
        return lax.ppermute(x, "tp", [(i, i ^ flip) for i in range(tp)])

    def inner(attn, w, res, gain):
        me = lax.axis_index("tp")
        rows_total, cols = res.shape
        pieces = {}
        dep = []
        near = None

        for t, (row, tm, col0, ncols, tn, splits) in enumerate(PLAN):
            if t == NEAR_AT:
                reps = rows_total // NEAR_ROWS
                other, own = products(attn, w, [(me ^ 1) * reps, me * reps], reps, NEAR_ROWS, 0, cols, 1024, (NEAR_ROWS,), dep)
                dep = [own]
                near = [own, send(other, 1)]
            per = rows_total // tm
            outs = products(attn, w, [(me ^ 2) * per + row // tm, (me ^ 3) * per + row // tm], 1, tm, col0, ncols, tn, splits, dep)
            dep = [outs[0]]
            for s, size in enumerate(splits):
                got = pieces.setdefault((row, size), ([], []))
                for b, flip in enumerate((2, 3)):
                    got[b].append(send(outs[b * len(splits) + s], flip))
                row += size

        gain2 = gain.reshape(1, cols)
        state = []
        for c, (row, size) in enumerate(sorted(pieces)):
            tr = min(size, 32)
            h, sq = add_rows(res, near, pieces[row, size], row, size, tr, col_groups, state[:1] if state else dep, c)
            state = norm_rows(h, sq, gain2, cols * col_groups, rows_total, row, tr, state)
        return tuple(state)

    row_spec = P(("dp", "tp"), "tp2")
    fn = jax.shard_map(inner, mesh=mesh, in_specs=(P("dp", "tp"), P("tp", "tp2"), row_spec, P("tp2")), out_specs=(row_spec, row_spec), check_vma=False)
    shapes = [jax.ShapeDtypeStruct(s, d) for s, d in (((4096, 16384), BF16), ((16384, 16384), BF16), ((4096, 16384), BF16), ((16384,), F32))]
    jax.eval_shape(fn, *shapes)
    return fn
```

```python
import jax
import jax.numpy as jnp
from jax import lax
from jax.experimental import pallas as pl
from jax.experimental.pallas import tpu as pltpu
from jax.sharding import PartitionSpec as P


EPS_NORM = 1e-6
F32, BF16 = jnp.float32, jnp.bfloat16
VMEM_BYTES = 67043328

ANY = pl.BlockSpec(memory_space=pl.ANY)
PARAMS = pltpu.CompilerParams(vmem_limit_bytes=VMEM_BYTES)
SMALL_VMEM = 50 * 2**20

BOTH = (2, 3)
PLAN = (
    ((2,), 0, 256, 0, 1024, 256, (256,)),
    ((3,), 0, 256, 0, 1024, 256, (256,)),
    (BOTH, 0, 256, 1024, 1536, 512, (256,)),
    (BOTH, 0, 256, 2560, 2560, 512, (256,)),
    (BOTH, 0, 256, 5120, 3072, 512, (256,)),
    (BOTH, 256, 256, 0, 8192, 512, (256,)),
    (BOTH, 512, 256, 0, 8192, 512, (256,)),
    (BOTH, 768, 256, 0, 8192, 512, (128, 80, 32, 16)),
)
NEAR_AT = 6
NEAR_ROWS = 256


def products(attn, w, blocks, reps, tm, col0, ncols, tn, splits, deps):
    depth = attn.shape[1]
    nb, ns = len(blocks), len(splits)

    def body(*refs):
        a_refs, w_ref = refs[nb:2 * nb], refs[2 * nb]
        outs = refs[2 * nb + 1 + len(deps):]
        for b in range(nb):
            val = jnp.dot(a_refs[b][...], w_ref[...], preferred_element_type=F32).astype(BF16)
            row = 0
            for s, size in enumerate(splits):
                outs[b * ns + s][...] = val[row:row + size]
                row += size

    c0 = col0 // tn
    a_specs = [pl.BlockSpec((tm, depth), lambda j, i, *idx, b=b: (idx[b][0] + i, 0)) for b in range(nb)]
    w_spec = pl.BlockSpec((depth, tn), lambda j, i, *idx: (0, c0 + j))
    out_specs = [pl.BlockSpec((size, tn), lambda j, i, *idx: (i, j)) for _ in range(nb) for size in splits]
    return pl.pallas_call(
        body,
        grid_spec=pltpu.PrefetchScalarGridSpec(
            num_scalar_prefetch=nb,
            grid=(ncols // tn, reps),
            in_specs=a_specs + [w_spec] + [ANY] * len(deps),
            out_specs=out_specs,
        ),
        out_shape=[jax.ShapeDtypeStruct((size * reps, ncols), BF16) for _ in range(nb) for size in splits],
        compiler_params=PARAMS,
        cost_estimate=pl.CostEstimate(
            flops=2 * nb * reps * tm * depth * ncols,
            bytes_accessed=2 * (depth * ncols + nb * reps * tm * (depth + ncols)),
            transcendentals=0),
    )(*[b.reshape(1).astype(jnp.int32) for b in blocks], *([attn] * nb), w, *deps)


def add_rows(res, near, far, row0, rows, tr, peers, deps, collective_id):
    cols = res.shape[1]
    nn, nf, per = len(near), len(far), len(far[0])
    widths = [piece.shape[1] for piece in far[0]]
    flat = [piece for group in far for piece in group]
    steps = rows // tr

    def body(*refs):
        r_ref, near_refs, far_refs = refs[0], refs[1:1 + nn], refs[1 + nn:1 + nn + nf * per]
        h_ref, sq_ref, mine, theirs, send_sem, recv_sem = refs[-6:]
        i = pl.program_id(0)
        peer = {"tp2": peers - 1 - lax.axis_index("tp2")}
        barrier = pltpu.get_barrier_semaphore()

        @pl.when(i == 0)
        def _():
            pl.semaphore_signal(barrier, inc=1, device_id=peer, device_id_type=pl.DeviceIdType.MESH)

        total = jnp.zeros((tr, 1), F32)
        base = 0
        for c, width in enumerate(widths):
            sl = slice(base, base + width)
            terms = [ref[:, sl] for ref in near_refs] + [far_refs[g * per + c][...] for g in range(nf)]
            y = terms[0].astype(F32)
            for term in terms[1:]:
                y = y + term.astype(F32)
            h = r_ref[:, sl].astype(F32) + y
            h_ref[:, sl] = h
            total = total + jnp.sum(h * h, axis=-1, keepdims=True)
            base += width
        mine[pl.ds(pl.multiple_of(i * tr, tr), tr), :] = jnp.broadcast_to(total, (tr, 128))

        @pl.when(i == steps - 1)
        def _():
            pl.semaphore_wait(barrier, 1)
            copy = pltpu.make_async_remote_copy(
                src_ref=mine, dst_ref=theirs, send_sem=send_sem, recv_sem=recv_sem,
                device_id=peer, device_id_type=pl.DeviceIdType.MESH)
            copy.start()
            copy.wait()
            sq_ref[...] = mine[...] + theirs[...]

    b0 = row0 // tr if near else 0
    full = pl.BlockSpec((tr, cols), lambda i: (b0 + i, 0))
    in_specs = [full] * (1 + nn) + [pl.BlockSpec((tr, piece.shape[1]), lambda i: (i, 0)) for piece in flat] + [ANY] * len(deps)
    return pl.pallas_call(
        body,
        grid=(steps,),
        in_specs=in_specs,
        out_specs=[pl.BlockSpec((tr, cols), lambda i: (i, 0)), pl.BlockSpec((rows, 128), lambda i: (0, 0))],
        out_shape=[jax.ShapeDtypeStruct((rows, cols), F32), jax.ShapeDtypeStruct((rows, 128), F32)],
        scratch_shapes=[
            pltpu.VMEM((rows, 128), F32),
            pltpu.VMEM((rows, 128), F32),
            pltpu.SemaphoreType.DMA,
            pltpu.SemaphoreType.DMA,
        ],
        compiler_params=pltpu.CompilerParams(vmem_limit_bytes=SMALL_VMEM, collective_id=collective_id, has_side_effects=True),
        cost_estimate=pl.CostEstimate(flops=8 * rows * cols, bytes_accessed=14 * rows * cols, transcendentals=0),
    )(res, *near, *flat, *deps)


def near_sum(res, near, row0, rows, deps):
    cols = res.shape[1]

    def body(*refs):
        total = refs[0][...].astype(F32)
        for ref in refs[1:1 + len(near)]:
            total = total + ref[...].astype(F32)
        refs[-1][...] = total

    return pl.pallas_call(
        body,
        grid=(1,),
        in_specs=[pl.BlockSpec((rows, cols), lambda i: (row0 // rows, 0))] * (1 + len(near)) + [ANY] * len(deps),
        out_specs=pl.BlockSpec((rows, cols), lambda i: (0, 0)),
        out_shape=jax.ShapeDtypeStruct((rows, cols), F32),
        compiler_params=pltpu.CompilerParams(vmem_limit_bytes=SMALL_VMEM),
        cost_estimate=pl.CostEstimate(flops=2 * rows * cols, bytes_accessed=10 * rows * cols, transcendentals=0),
    )(res, *near, *deps)


def norm_rows(h, sq, gain, width, total_rows, row0, tr, state):
    rows, cols = h.shape

    def body(*refs):
        h_ref, sq_ref, g_ref, ho_ref, n_ref = refs[0], refs[1], refs[2], refs[-2], refs[-1]
        inv = lax.rsqrt(sq_ref[:, :1] / width + EPS_NORM)
        h = h_ref[...]
        ho_ref[...] = h.astype(BF16)
        n_ref[...] = (h * inv * g_ref[...]).astype(BF16)

    b0 = row0 // tr
    in_specs = [
        pl.BlockSpec((tr, cols), lambda i: (i, 0)),
        pl.BlockSpec((tr, 128), lambda i: (i, 0)),
        pl.BlockSpec((1, cols), lambda i: (0, 0)),
    ] + [ANY] * len(state)
    out = jax.ShapeDtypeStruct((total_rows, cols), BF16)
    return pl.pallas_call(
        body,
        grid=(rows // tr,),
        in_specs=in_specs,
        out_specs=[pl.BlockSpec((tr, cols), lambda i: (b0 + i, 0))] * 2,
        out_shape=[out, out],
        input_output_aliases={3 + i: i for i in range(len(state))},
        compiler_params=pltpu.CompilerParams(vmem_limit_bytes=SMALL_VMEM),
        cost_estimate=pl.CostEstimate(flops=4 * rows * cols, bytes_accessed=8 * rows * cols, transcendentals=0),
    )(h, sq, gain, *state)


def solution(mesh):
    tp = mesh.shape["tp"]
    col_groups = mesh.shape["tp2"]

    def send(x, flip):
        return lax.ppermute(x, "tp", [(i, i ^ flip) for i in range(tp)])

    def inner(attn, w, res, gain):
        me = lax.axis_index("tp")
        rows_total, cols = res.shape
        pieces = {}
        dep = []
        near = None

        for t, (flips, row, tm, col0, ncols, tn, splits) in enumerate(PLAN):
            if t == NEAR_AT:
                reps = rows_total // NEAR_ROWS
                other, own = products(attn, w, [(me ^ 1) * reps, me * reps], reps, NEAR_ROWS, 0, cols, 1024, (NEAR_ROWS,), dep)
                dep = [own]
                near = [own, send(other, 1)]
            per = rows_total // tm
            outs = products(attn, w, [(me ^ flip) * per + row // tm for flip in flips], 1, tm, col0, ncols, tn, splits, dep)
            dep = [outs[0]]
            for s, size in enumerate(splits):
                got = pieces.setdefault((row, size), ([], []))
                for b, flip in enumerate(flips):
                    got[BOTH.index(flip)].append(send(outs[b * len(splits) + s], flip))
                row += size

        gain2 = gain.reshape(1, cols)
        state = []
        chunks = sorted(pieces)
        for c, (row, size) in enumerate(chunks):
            tr = 32 if (row | size) % 32 == 0 else 16
            if c == 1:
                ready = near_sum(res, near, *chunks[-1], state[:1])
            terms = (res, near) if c < len(chunks) - 1 else (ready, [])
            h, sq = add_rows(*terms, pieces[row, size], row, size, tr, col_groups, state[:1] if state else dep, c)
            state = norm_rows(h, sq, gain2, cols * col_groups, rows_total, row, tr, state)
        return tuple(state)

    row_spec = P(("dp", "tp"), "tp2")
    fn = jax.shard_map(inner, mesh=mesh, in_specs=(P("dp", "tp"), P("tp", "tp2"), row_spec, P("tp2")), out_specs=(row_spec, row_spec), check_vma=False)
    shapes = [jax.ShapeDtypeStruct(s, d) for s, d in (((4096, 16384), BF16), ((16384, 16384), BF16), ((4096, 16384), BF16), ((16384,), F32))]
    jax.eval_shape(fn, *shapes)
    return fn
```

```python
import jax
import jax.numpy as jnp
from jax import lax
from jax.experimental import pallas as pl
from jax.experimental.pallas import tpu as pltpu
from jax.sharding import PartitionSpec as P


EPS_NORM = 1e-6
F32, BF16 = jnp.float32, jnp.bfloat16
VMEM_BYTES = 67043328

ANY = pl.BlockSpec(memory_space=pl.ANY)
PARAMS = pltpu.CompilerParams(vmem_limit_bytes=VMEM_BYTES)
SMALL_VMEM = 50 * 2**20

HEAD_ROWS = 256
HEAD_TILE = 256
HEAD_LAG = 6
BOTH = (2, 3)
PLAN = (
    ((3,), 0, 256, (256,)),
    ((3,), 256, 256, (256,)),
    (BOTH, 512, 256, (256,)),
    (BOTH, 768, 256, (128, 80, 32, 16)),
)
NEAR_AT = 2
NEAR_ROWS = 256


def head(attn, w, tp, rows_total, collective_id):
    depth, cols = w.shape
    tiles = cols // HEAD_TILE

    def far():
        return lax.rem(lax.axis_index("tp") + 2, tp)

    def body(a_ref, w_ref, got_ref, y_ref, held, send_sem, recv_sem):
        j = pl.program_id(0)
        peer = {"tp": far()}
        lag = (1 - lax.rem(lax.axis_index("tp"), 2)) * HEAD_LAG

        def copy(t, row=0, rows=HEAD_ROWS, sem=None):
            sem = t if sem is None else sem
            return pltpu.make_async_remote_copy(
                src_ref=held.at[t, pl.ds(row, rows)],
                dst_ref=got_ref.at[pl.ds(row, rows), pl.ds(pl.multiple_of(t * HEAD_TILE, HEAD_TILE), HEAD_TILE)],
                send_sem=send_sem.at[sem],
                recv_sem=recv_sem.at[sem],
                device_id=peer,
                device_id_type=pl.DeviceIdType.MESH,
            )

        half = HEAD_ROWS // 2
        upper, lower = copy(0, 0, half, 0), copy(0, half, half, tiles)
        barrier = pltpu.get_barrier_semaphore()

        @pl.when(j == 0)
        def _():
            pl.semaphore_signal(barrier, inc=1, device_id=peer, device_id_type=pl.DeviceIdType.MESH)

        val = jnp.dot(a_ref[:half], w_ref[...], preferred_element_type=F32).astype(BF16)

        @pl.when(j == 0)
        def _():
            pl.semaphore_wait(barrier, 1)

        @pl.when(j < tiles)
        def _():
            held[j, :half] = val

        @pl.when(j >= tiles)
        def _():
            y_ref[:half] = val

        @pl.when((j == 0) & (lag == 0))
        def _():
            upper.start()

        val2 = jnp.dot(a_ref[half:], w_ref[...], preferred_element_type=F32).astype(BF16)

        @pl.when(j < tiles)
        def _():
            held[j, half:] = val2

            @pl.when((j == 0) & (lag == 0))
            def _():
                lower.start()

            @pl.when((j > 0) & (j == lag))
            def _():
                upper.start()
                lower.start()
                lax.fori_loop(1, lag, lambda t, c: (copy(t).start(), c)[1], 0)

            @pl.when((j > 0) & (j >= lag))
            def _():
                copy(j).start()

        @pl.when(j >= tiles)
        def _():
            y_ref[half:] = val2

        @pl.when(j == 2 * tiles - 1)
        def _():
            upper.wait()
            lower.wait()
            lax.fori_loop(1, tiles, lambda t, c: (copy(t).wait(), c)[1], 0)

    per = rows_total // HEAD_ROWS
    return pl.pallas_call(
        body,
        grid=(2 * tiles,),
        in_specs=[
            pl.BlockSpec((HEAD_ROWS, depth), lambda j: (far() * per + j // tiles, 0)),
            pl.BlockSpec((depth, HEAD_TILE), lambda j: (0, lax.rem(j, tiles))),
        ],
        out_specs=[ANY, pl.BlockSpec((HEAD_ROWS, HEAD_TILE), lambda j: (0, jnp.maximum(j - tiles, 0)))],
        out_shape=[jax.ShapeDtypeStruct((HEAD_ROWS, cols), BF16)] * 2,
        scratch_shapes=[
            pltpu.VMEM((tiles, HEAD_ROWS, HEAD_TILE), BF16),
            pltpu.SemaphoreType.DMA((tiles + 1,)),
            pltpu.SemaphoreType.DMA((tiles + 1,)),
        ],
        compiler_params=pltpu.CompilerParams(vmem_limit_bytes=VMEM_BYTES, collective_id=collective_id, has_side_effects=True),
        cost_estimate=pl.CostEstimate(flops=4 * HEAD_ROWS * depth * cols, bytes_accessed=4 * depth * cols, transcendentals=0),
        name="head",
    )(attn, w)


def products(attn, w, blocks, reps, tm, col0, ncols, tn, splits, deps):
    depth = attn.shape[1]
    nb, ns = len(blocks), len(splits)

    def body(*refs):
        a_refs, w_ref = refs[nb:2 * nb], refs[2 * nb]
        outs = refs[2 * nb + 1 + len(deps):]
        for b in range(nb):
            val = jnp.dot(a_refs[b][...], w_ref[...], preferred_element_type=F32).astype(BF16)
            row = 0
            for s, size in enumerate(splits):
                outs[b * ns + s][...] = val[row:row + size]
                row += size

    c0 = col0 // tn
    a_specs = [pl.BlockSpec((tm, depth), lambda j, i, *idx, b=b: (idx[b][0] + i, 0)) for b in range(nb)]
    w_spec = pl.BlockSpec((depth, tn), lambda j, i, *idx: (0, c0 + j))
    out_specs = [pl.BlockSpec((size, tn), lambda j, i, *idx: (i, j)) for _ in range(nb) for size in splits]
    return pl.pallas_call(
        body,
        grid_spec=pltpu.PrefetchScalarGridSpec(
            num_scalar_prefetch=nb,
            grid=(ncols // tn, reps),
            in_specs=a_specs + [w_spec] + [ANY] * len(deps),
            out_specs=out_specs,
        ),
        out_shape=[jax.ShapeDtypeStruct((size * reps, ncols), BF16) for _ in range(nb) for size in splits],
        compiler_params=PARAMS,
        cost_estimate=pl.CostEstimate(
            flops=2 * nb * reps * tm * depth * ncols,
            bytes_accessed=2 * (depth * ncols + nb * reps * tm * (depth + ncols)),
            transcendentals=0),
    )(*[b.reshape(1).astype(jnp.int32) for b in blocks], *([attn] * nb), w, *deps)


def add_rows(res, near, far, row0, rows, tr, peers, deps, collective_id):
    cols = res.shape[1]
    nn, nf, per = len(near), len(far), len(far[0])
    widths = [piece.shape[1] for piece in far[0]]
    flat = [piece for group in far for piece in group]
    steps = rows // tr

    def body(*refs):
        r_ref, near_refs, far_refs = refs[0], refs[1:1 + nn], refs[1 + nn:1 + nn + nf * per]
        h_ref, sq_ref, mine, theirs, send_sem, recv_sem = refs[-6:]
        i = pl.program_id(0)
        peer = {"tp2": peers - 1 - lax.axis_index("tp2")}
        barrier = pltpu.get_barrier_semaphore()

        @pl.when(i == 0)
        def _():
            pl.semaphore_signal(barrier, inc=1, device_id=peer, device_id_type=pl.DeviceIdType.MESH)

        total = jnp.zeros((tr, 1), F32)
        base = 0
        for c, width in enumerate(widths):
            sl = slice(base, base + width)
            terms = [ref[:, sl] for ref in near_refs] + [far_refs[g * per + c][...] for g in range(nf)]
            y = terms[0].astype(F32)
            for term in terms[1:]:
                y = y + term.astype(F32)
            h = r_ref[:, sl].astype(F32) + y
            h_ref[:, sl] = h
            total = total + jnp.sum(h * h, axis=-1, keepdims=True)
            base += width
        mine[pl.ds(pl.multiple_of(i * tr, tr), tr), :] = jnp.broadcast_to(total, (tr, 128))

        @pl.when(i == steps - 1)
        def _():
            pl.semaphore_wait(barrier, 1)
            copy = pltpu.make_async_remote_copy(
                src_ref=mine, dst_ref=theirs, send_sem=send_sem, recv_sem=recv_sem,
                device_id=peer, device_id_type=pl.DeviceIdType.MESH)
            copy.start()
            copy.wait()
            sq_ref[...] = mine[...] + theirs[...]

    b0 = row0 // tr if near else 0
    full = pl.BlockSpec((tr, cols), lambda i: (b0 + i, 0))
    in_specs = [full] * (1 + nn) + [pl.BlockSpec((tr, piece.shape[1]), lambda i: (i, 0)) for piece in flat] + [ANY] * len(deps)
    return pl.pallas_call(
        body,
        grid=(steps,),
        in_specs=in_specs,
        out_specs=[pl.BlockSpec((tr, cols), lambda i: (i, 0)), pl.BlockSpec((rows, 128), lambda i: (0, 0))],
        out_shape=[jax.ShapeDtypeStruct((rows, cols), F32), jax.ShapeDtypeStruct((rows, 128), F32)],
        scratch_shapes=[
            pltpu.VMEM((rows, 128), F32),
            pltpu.VMEM((rows, 128), F32),
            pltpu.SemaphoreType.DMA,
            pltpu.SemaphoreType.DMA,
        ],
        compiler_params=pltpu.CompilerParams(vmem_limit_bytes=SMALL_VMEM, collective_id=collective_id, has_side_effects=True),
        cost_estimate=pl.CostEstimate(flops=8 * rows * cols, bytes_accessed=14 * rows * cols, transcendentals=0),
    )(res, *near, *flat, *deps)


def near_sum(res, near, row0, rows, deps):
    cols = res.shape[1]

    def body(*refs):
        total = refs[0][...].astype(F32)
        for ref in refs[1:1 + len(near)]:
            total = total + ref[...].astype(F32)
        refs[-1][...] = total

    return pl.pallas_call(
        body,
        grid=(1,),
        in_specs=[pl.BlockSpec((rows, cols), lambda i: (row0 // rows, 0))] * (1 + len(near)) + [ANY] * len(deps),
        out_specs=pl.BlockSpec((rows, cols), lambda i: (0, 0)),
        out_shape=jax.ShapeDtypeStruct((rows, cols), F32),
        compiler_params=pltpu.CompilerParams(vmem_limit_bytes=SMALL_VMEM),
        cost_estimate=pl.CostEstimate(flops=2 * rows * cols, bytes_accessed=10 * rows * cols, transcendentals=0),
    )(res, *near, *deps)


def norm_rows(h, sq, gain, width, total_rows, row0, tr, state):
    rows, cols = h.shape

    def body(*refs):
        h_ref, sq_ref, g_ref, ho_ref, n_ref = refs[0], refs[1], refs[2], refs[-2], refs[-1]
        inv = lax.rsqrt(sq_ref[:, :1] / width + EPS_NORM)
        h = h_ref[...]
        ho_ref[...] = h.astype(BF16)
        n_ref[...] = (h * inv * g_ref[...]).astype(BF16)

    b0 = row0 // tr
    in_specs = [
        pl.BlockSpec((tr, cols), lambda i: (i, 0)),
        pl.BlockSpec((tr, 128), lambda i: (i, 0)),
        pl.BlockSpec((1, cols), lambda i: (0, 0)),
    ] + [ANY] * len(state)
    out = jax.ShapeDtypeStruct((total_rows, cols), BF16)
    return pl.pallas_call(
        body,
        grid=(rows // tr,),
        in_specs=in_specs,
        out_specs=[pl.BlockSpec((tr, cols), lambda i: (b0 + i, 0))] * 2,
        out_shape=[out, out],
        input_output_aliases={3 + i: i for i in range(len(state))},
        compiler_params=pltpu.CompilerParams(vmem_limit_bytes=SMALL_VMEM),
        cost_estimate=pl.CostEstimate(flops=4 * rows * cols, bytes_accessed=8 * rows * cols, transcendentals=0),
    )(h, sq, gain, *state)


def solution(mesh):
    tp = mesh.shape["tp"]
    col_groups = mesh.shape["tp2"]

    def send(x, flip):
        return lax.ppermute(x, "tp", [(i, i ^ flip) for i in range(tp)])

    def inner(attn, w, res, gain):
        me = lax.axis_index("tp")
        rows_total, cols = res.shape
        pieces = {}
        near = None

        got, y = head(attn, w, tp, rows_total, 7)
        pieces[0, HEAD_ROWS] = ([got], [])
        pieces[HEAD_ROWS, HEAD_ROWS] = ([send(y, 2)], [])
        dep = [y]
        for t, (flips, row, tm, splits) in enumerate(PLAN):
            if t == NEAR_AT:
                reps = rows_total // NEAR_ROWS
                other, own = products(attn, w, [(me ^ 1) * reps, me * reps], reps, NEAR_ROWS, 0, cols, 1024, (NEAR_ROWS,), dep)
                dep = [own]
                near = [own, send(other, 1)]
            per = rows_total // tm
            outs = products(attn, w, [(me ^ flip) * per + row // tm for flip in flips], 1, tm, 0, cols, 512, splits, dep)
            dep = [outs[0]]
            for s, size in enumerate(splits):
                into = pieces.setdefault((row, size), ([], []))
                for b, flip in enumerate(flips):
                    into[BOTH.index(flip)].append(send(outs[b * len(splits) + s], flip))
                row += size

        gain2 = gain.reshape(1, cols)
        state = []
        chunks = sorted(pieces)
        for c, (row, size) in enumerate(chunks):
            tr = 32 if (row | size) % 32 == 0 else 16
            if c == 1:
                ready = near_sum(res, near, *chunks[-1], state[:1])
            terms = (res, near) if c < len(chunks) - 1 else (ready, [])
            h, sq = add_rows(*terms, pieces[row, size], row, size, tr, col_groups, state[:1] if state else dep, c)
            state = norm_rows(h, sq, gain2, cols * col_groups, rows_total, row, tr, state)
        return tuple(state)

    row_spec = P(("dp", "tp"), "tp2")
    fn = jax.shard_map(inner, mesh=mesh, in_specs=(P("dp", "tp"), P("tp", "tp2"), row_spec, P("tp2")), out_specs=(row_spec, row_spec), check_vma=False)
    shapes = [jax.ShapeDtypeStruct(s, d) for s, d in (((4096, 16384), BF16), ((16384, 16384), BF16), ((4096, 16384), BF16), ((16384,), F32))]
    jax.eval_shape(fn, *shapes)
    return fn
```

```python
import jax
import jax.numpy as jnp
from jax import lax
from jax.experimental import pallas as pl
from jax.experimental.pallas import tpu as pltpu
from jax.sharding import PartitionSpec as P


EPS_NORM = 1e-6
F32, BF16 = jnp.float32, jnp.bfloat16
VMEM_BYTES = 67043328

ANY = pl.BlockSpec(memory_space=pl.ANY)
PARAMS = pltpu.CompilerParams(vmem_limit_bytes=VMEM_BYTES)
SMALL_VMEM = 50 * 2**20

HEAD_ROWS = 256
HEAD_TILE = 256
HEAD_LAG = 6
BOTH = (2, 3)
PLAN = (
    ((3,), 0, 256, (256,)),
    ((3,), 256, 256, (256,)),
    (BOTH, 512, 256, (256,)),
    (BOTH, 768, 256, (128, 80, 32, 16)),
)
NEAR_AT = 3
NEAR_ROWS = 256


def head(attn, w, tp, rows_total, collective_id):
    depth, cols = w.shape
    tiles = cols // HEAD_TILE

    def far():
        return lax.rem(lax.axis_index("tp") + 2, tp)

    def body(a_ref, w_ref, got_ref, y_ref, held, send_sem, recv_sem):
        j = pl.program_id(0)
        peer = {"tp": far()}
        lag = (1 - lax.rem(lax.axis_index("tp"), 2)) * HEAD_LAG

        def copy(t):
            return pltpu.make_async_remote_copy(
                src_ref=held.at[t],
                dst_ref=got_ref.at[:, pl.ds(pl.multiple_of(t * HEAD_TILE, HEAD_TILE), HEAD_TILE)],
                send_sem=send_sem.at[t],
                recv_sem=recv_sem.at[t],
                device_id=peer,
                device_id_type=pl.DeviceIdType.MESH,
            )

        barrier = pltpu.get_barrier_semaphore()

        @pl.when(j == 0)
        def _():
            pl.semaphore_signal(barrier, inc=1, device_id=peer, device_id_type=pl.DeviceIdType.MESH)

        val = jnp.dot(a_ref[...], w_ref[...], preferred_element_type=F32).astype(BF16)

        @pl.when(j == 0)
        def _():
            pl.semaphore_wait(barrier, 1)

        @pl.when(j < tiles)
        def _():
            held[j] = val

            @pl.when(j == lag)
            def _():
                lax.fori_loop(0, lag, lambda t, c: (copy(t).start(), c)[1], 0)

            @pl.when(j >= lag)
            def _():
                copy(j).start()

        @pl.when(j >= tiles)
        def _():
            y_ref[...] = val

        @pl.when(j == 2 * tiles - 1)
        def _():
            lax.fori_loop(0, tiles, lambda t, c: (copy(t).wait(), c)[1], 0)

    per = rows_total // HEAD_ROWS
    return pl.pallas_call(
        body,
        grid=(2 * tiles,),
        in_specs=[
            pl.BlockSpec((HEAD_ROWS, depth), lambda j: (far() * per + j // tiles, 0)),
            pl.BlockSpec((depth, HEAD_TILE), lambda j: (0, lax.rem(j, tiles))),
        ],
        out_specs=[ANY, pl.BlockSpec((HEAD_ROWS, HEAD_TILE), lambda j: (0, jnp.maximum(j - tiles, 0)))],
        out_shape=[jax.ShapeDtypeStruct((HEAD_ROWS, cols), BF16)] * 2,
        scratch_shapes=[
            pltpu.VMEM((tiles, HEAD_ROWS, HEAD_TILE), BF16),
            pltpu.SemaphoreType.DMA((tiles,)),
            pltpu.SemaphoreType.DMA((tiles,)),
        ],
        compiler_params=pltpu.CompilerParams(vmem_limit_bytes=VMEM_BYTES, collective_id=collective_id, has_side_effects=True),
        cost_estimate=pl.CostEstimate(flops=4 * HEAD_ROWS * depth * cols, bytes_accessed=4 * depth * cols, transcendentals=0),
        name="head",
    )(attn, w)


def products(attn, w, blocks, reps, tm, col0, ncols, tn, splits, deps):
    depth = attn.shape[1]
    nb, ns = len(blocks), len(splits)

    def body(*refs):
        a_refs, w_ref = refs[nb:2 * nb], refs[2 * nb]
        outs = refs[2 * nb + 1 + len(deps):]
        for b in range(nb):
            val = jnp.dot(a_refs[b][...], w_ref[...], preferred_element_type=F32).astype(BF16)
            row = 0
            for s, size in enumerate(splits):
                outs[b * ns + s][...] = val[row:row + size]
                row += size

    c0 = col0 // tn
    a_specs = [pl.BlockSpec((tm, depth), lambda j, i, *idx, b=b: (idx[b][0] + i, 0)) for b in range(nb)]
    w_spec = pl.BlockSpec((depth, tn), lambda j, i, *idx: (0, c0 + j))
    out_specs = [pl.BlockSpec((size, tn), lambda j, i, *idx: (i, j)) for _ in range(nb) for size in splits]
    return pl.pallas_call(
        body,
        grid_spec=pltpu.PrefetchScalarGridSpec(
            num_scalar_prefetch=nb,
            grid=(ncols // tn, reps),
            in_specs=a_specs + [w_spec] + [ANY] * len(deps),
            out_specs=out_specs,
        ),
        out_shape=[jax.ShapeDtypeStruct((size * reps, ncols), BF16) for _ in range(nb) for size in splits],
        compiler_params=PARAMS,
        cost_estimate=pl.CostEstimate(
            flops=2 * nb * reps * tm * depth * ncols,
            bytes_accessed=2 * (depth * ncols + nb * reps * tm * (depth + ncols)),
            transcendentals=0),
    )(*[b.reshape(1).astype(jnp.int32) for b in blocks], *([attn] * nb), w, *deps)


def add_rows(res, near, far, row0, rows, tr, peers, deps, collective_id):
    cols = res.shape[1]
    nn, nf, per = len(near), len(far), len(far[0])
    widths = [piece.shape[1] for piece in far[0]]
    flat = [piece for group in far for piece in group]
    steps = rows // tr

    def body(*refs):
        r_ref, near_refs, far_refs = refs[0], refs[1:1 + nn], refs[1 + nn:1 + nn + nf * per]
        h_ref, sq_ref, mine, theirs, send_sem, recv_sem = refs[-6:]
        i = pl.program_id(0)
        peer = {"tp2": peers - 1 - lax.axis_index("tp2")}
        barrier = pltpu.get_barrier_semaphore()

        @pl.when(i == 0)
        def _():
            pl.semaphore_signal(barrier, inc=1, device_id=peer, device_id_type=pl.DeviceIdType.MESH)

        total = jnp.zeros((tr, 1), F32)
        base = 0
        for c, width in enumerate(widths):
            sl = slice(base, base + width)
            terms = [ref[:, sl] for ref in near_refs] + [far_refs[g * per + c][...] for g in range(nf)]
            y = terms[0].astype(F32)
            for term in terms[1:]:
                y = y + term.astype(F32)
            h = r_ref[:, sl].astype(F32) + y
            h_ref[:, sl] = h
            total = total + jnp.sum(h * h, axis=-1, keepdims=True)
            base += width
        mine[pl.ds(pl.multiple_of(i * tr, tr), tr), :] = jnp.broadcast_to(total, (tr, 128))

        @pl.when(i == steps - 1)
        def _():
            pl.semaphore_wait(barrier, 1)
            copy = pltpu.make_async_remote_copy(
                src_ref=mine, dst_ref=theirs, send_sem=send_sem, recv_sem=recv_sem,
                device_id=peer, device_id_type=pl.DeviceIdType.MESH)
            copy.start()
            copy.wait()
            sq_ref[...] = mine[...] + theirs[...]

    b0 = row0 // tr if near else 0
    full = pl.BlockSpec((tr, cols), lambda i: (b0 + i, 0))
    in_specs = [full] * (1 + nn) + [pl.BlockSpec((tr, piece.shape[1]), lambda i: (i, 0)) for piece in flat] + [ANY] * len(deps)
    return pl.pallas_call(
        body,
        grid=(steps,),
        in_specs=in_specs,
        out_specs=[pl.BlockSpec((tr, cols), lambda i: (i, 0)), pl.BlockSpec((rows, 128), lambda i: (0, 0))],
        out_shape=[jax.ShapeDtypeStruct((rows, cols), F32), jax.ShapeDtypeStruct((rows, 128), F32)],
        scratch_shapes=[
            pltpu.VMEM((rows, 128), F32),
            pltpu.VMEM((rows, 128), F32),
            pltpu.SemaphoreType.DMA,
            pltpu.SemaphoreType.DMA,
        ],
        compiler_params=pltpu.CompilerParams(vmem_limit_bytes=SMALL_VMEM, collective_id=collective_id, has_side_effects=True),
        cost_estimate=pl.CostEstimate(flops=8 * rows * cols, bytes_accessed=14 * rows * cols, transcendentals=0),
    )(res, *near, *flat, *deps)


def near_sum(res, near, row0, rows, deps):
    cols = res.shape[1]

    def body(*refs):
        total = refs[0][...].astype(F32)
        for ref in refs[1:1 + len(near)]:
            total = total + ref[...].astype(F32)
        refs[-1][...] = total

    return pl.pallas_call(
        body,
        grid=(1,),
        in_specs=[pl.BlockSpec((rows, cols), lambda i: (row0 // rows, 0))] * (1 + len(near)) + [ANY] * len(deps),
        out_specs=pl.BlockSpec((rows, cols), lambda i: (0, 0)),
        out_shape=jax.ShapeDtypeStruct((rows, cols), F32),
        compiler_params=pltpu.CompilerParams(vmem_limit_bytes=SMALL_VMEM),
        cost_estimate=pl.CostEstimate(flops=2 * rows * cols, bytes_accessed=10 * rows * cols, transcendentals=0),
    )(res, *near, *deps)


def norm_rows(h, sq, gain, width, total_rows, row0, tr, state):
    rows, cols = h.shape

    def body(*refs):
        h_ref, sq_ref, g_ref, ho_ref, n_ref = refs[0], refs[1], refs[2], refs[-2], refs[-1]
        inv = lax.rsqrt(sq_ref[:, :1] / width + EPS_NORM)
        h = h_ref[...]
        ho_ref[...] = h.astype(BF16)
        n_ref[...] = (h * inv * g_ref[...]).astype(BF16)

    b0 = row0 // tr
    in_specs = [
        pl.BlockSpec((tr, cols), lambda i: (i, 0)),
        pl.BlockSpec((tr, 128), lambda i: (i, 0)),
        pl.BlockSpec((1, cols), lambda i: (0, 0)),
    ] + [ANY] * len(state)
    out = jax.ShapeDtypeStruct((total_rows, cols), BF16)
    return pl.pallas_call(
        body,
        grid=(rows // tr,),
        in_specs=in_specs,
        out_specs=[pl.BlockSpec((tr, cols), lambda i: (b0 + i, 0))] * 2,
        out_shape=[out, out],
        input_output_aliases={3 + i: i for i in range(len(state))},
        compiler_params=pltpu.CompilerParams(vmem_limit_bytes=SMALL_VMEM),
        cost_estimate=pl.CostEstimate(flops=4 * rows * cols, bytes_accessed=8 * rows * cols, transcendentals=0),
    )(h, sq, gain, *state)


def solution(mesh):
    tp = mesh.shape["tp"]
    col_groups = mesh.shape["tp2"]

    def send(x, flip):
        return lax.ppermute(x, "tp", [(i, i ^ flip) for i in range(tp)])

    def inner(attn, w, res, gain):
        me = lax.axis_index("tp")
        rows_total, cols = res.shape
        pieces = {}
        near = None

        got, y = head(attn, w, tp, rows_total, 7)
        pieces[0, HEAD_ROWS] = ([got], [])
        pieces[HEAD_ROWS, HEAD_ROWS] = ([send(y, 2)], [])
        dep = [y]
        for t, (flips, row, tm, splits) in enumerate(PLAN):
            if t == NEAR_AT:
                reps = rows_total // NEAR_ROWS
                other, own = products(attn, w, [(me ^ 1) * reps, me * reps], reps, NEAR_ROWS, 0, cols, 1024, (NEAR_ROWS,), dep)
                dep = [own]
                near = [own, send(other, 1)]
            per = rows_total // tm
            outs = products(attn, w, [(me ^ flip) * per + row // tm for flip in flips], 1, tm, 0, cols, 512, splits, dep)
            dep = [outs[0]]
            for s, size in enumerate(splits):
                into = pieces.setdefault((row, size), ([], []))
                for b, flip in enumerate(flips):
                    into[BOTH.index(flip)].append(send(outs[b * len(splits) + s], flip))
                row += size

        gain2 = gain.reshape(1, cols)
        state = []
        chunks = sorted(pieces)
        for c, (row, size) in enumerate(chunks):
            tr = 32 if (row | size) % 32 == 0 else 16
            if c == 1:
                ready = near_sum(res, near, *chunks[-1], state[:1])
            terms = (res, near) if c < len(chunks) - 1 else (ready, [])
            h, sq = add_rows(*terms, pieces[row, size], row, size, tr, col_groups, state[:1] if state else dep, c)
            state = norm_rows(h, sq, gain2, cols * col_groups, rows_total, row, tr, state)
        return tuple(state)

    row_spec = P(("dp", "tp"), "tp2")
    fn = jax.shard_map(inner, mesh=mesh, in_specs=(P("dp", "tp"), P("tp", "tp2"), row_spec, P("tp2")), out_specs=(row_spec, row_spec), check_vma=False)
    shapes = [jax.ShapeDtypeStruct(s, d) for s, d in (((4096, 16384), BF16), ((16384, 16384), BF16), ((4096, 16384), BF16), ((16384,), F32))]
    jax.eval_shape(fn, *shapes)
    return fn
```

```python
import jax
import jax.numpy as jnp
from jax import lax
from jax.experimental import pallas as pl
from jax.experimental.pallas import tpu as pltpu
from jax.sharding import PartitionSpec as P


EPS_NORM = 1e-6
F32, BF16 = jnp.float32, jnp.bfloat16
VMEM_BYTES = 67043328

ANY = pl.BlockSpec(memory_space=pl.ANY)
PARAMS = pltpu.CompilerParams(vmem_limit_bytes=VMEM_BYTES)
SMALL_VMEM = 50 * 2**20

HEAD_ROWS = 256
HEAD_TILE = 256
HEAD_LAG = 6
BOTH = (2, 3)
PLAN = (
    ((3,), 0, 256, (256,)),
    ((3,), 256, 256, (256,)),
    (BOTH, 512, 256, (256,)),
    (BOTH, 768, 256, (128, 80, 32, 16)),
)
NEAR_AT = 3
NEAR_ROWS = 256


def head(attn, w, tp, rows_total, collective_id):
    depth, cols = w.shape
    tiles = cols // HEAD_TILE

    def far():
        return lax.rem(lax.axis_index("tp") + 2, tp)

    def body(a_ref, w_ref, got_ref, y_ref, held, send_sem, recv_sem):
        j = pl.program_id(0)
        peer = {"tp": far()}
        lag = (1 - lax.rem(lax.axis_index("tp"), 2)) * HEAD_LAG

        def copy(t):
            return pltpu.make_async_remote_copy(
                src_ref=held.at[t],
                dst_ref=got_ref.at[:, pl.ds(pl.multiple_of(t * HEAD_TILE, HEAD_TILE), HEAD_TILE)],
                send_sem=send_sem.at[t],
                recv_sem=recv_sem.at[t],
                device_id=peer,
                device_id_type=pl.DeviceIdType.MESH,
            )

        barrier = pltpu.get_barrier_semaphore()

        @pl.when(j == 0)
        def _():
            pl.semaphore_signal(barrier, inc=1, device_id=peer, device_id_type=pl.DeviceIdType.MESH)

        val = jnp.dot(a_ref[...], w_ref[...], preferred_element_type=F32).astype(BF16)

        @pl.when(j == 0)
        def _():
            pl.semaphore_wait(barrier, 1)

        @pl.when(j < tiles)
        def _():
            held[j] = val

            @pl.when(j == lag)
            def _():
                lax.fori_loop(0, lag, lambda t, c: (copy(t).start(), c)[1], 0)

            @pl.when(j >= lag)
            def _():
                copy(j).start()

        @pl.when(j >= tiles)
        def _():
            y_ref[...] = val

        @pl.when(j == 2 * tiles - 1)
        def _():
            lax.fori_loop(0, tiles, lambda t, c: (copy(t).wait(), c)[1], 0)

    per = rows_total // HEAD_ROWS
    return pl.pallas_call(
        body,
        grid=(2 * tiles,),
        in_specs=[
            pl.BlockSpec((HEAD_ROWS, depth), lambda j: (far() * per + j // tiles, 0)),
            pl.BlockSpec((depth, HEAD_TILE), lambda j: (0, lax.rem(j, tiles))),
        ],
        out_specs=[ANY, pl.BlockSpec((HEAD_ROWS, HEAD_TILE), lambda j: (0, jnp.maximum(j - tiles, 0)))],
        out_shape=[jax.ShapeDtypeStruct((HEAD_ROWS, cols), BF16)] * 2,
        scratch_shapes=[
            pltpu.VMEM((tiles, HEAD_ROWS, HEAD_TILE), BF16),
            pltpu.SemaphoreType.DMA((tiles,)),
            pltpu.SemaphoreType.DMA((tiles,)),
        ],
        compiler_params=pltpu.CompilerParams(vmem_limit_bytes=VMEM_BYTES, collective_id=collective_id, has_side_effects=True),
        cost_estimate=pl.CostEstimate(flops=4 * HEAD_ROWS * depth * cols, bytes_accessed=4 * depth * cols, transcendentals=0),
        name="head",
    )(attn, w)


def products(attn, w, blocks, reps, tm, col0, ncols, tn, splits, deps):
    depth = attn.shape[1]
    nb, ns = len(blocks), len(splits)

    def body(*refs):
        a_refs, w_ref = refs[nb:2 * nb], refs[2 * nb]
        outs = refs[2 * nb + 1 + len(deps):]
        for b in range(nb):
            val = jnp.dot(a_refs[b][...], w_ref[...], preferred_element_type=F32).astype(BF16)
            row = 0
            for s, size in enumerate(splits):
                outs[b * ns + s][...] = val[row:row + size]
                row += size

    c0 = col0 // tn
    a_specs = [pl.BlockSpec((tm, depth), lambda j, i, *idx, b=b: (idx[b][0] + i, 0)) for b in range(nb)]
    w_spec = pl.BlockSpec((depth, tn), lambda j, i, *idx: (0, c0 + j))
    out_specs = [pl.BlockSpec((size, tn), lambda j, i, *idx: (i, j)) for _ in range(nb) for size in splits]
    return pl.pallas_call(
        body,
        grid_spec=pltpu.PrefetchScalarGridSpec(
            num_scalar_prefetch=nb,
            grid=(ncols // tn, reps),
            in_specs=a_specs + [w_spec] + [ANY] * len(deps),
            out_specs=out_specs,
        ),
        out_shape=[jax.ShapeDtypeStruct((size * reps, ncols), BF16) for _ in range(nb) for size in splits],
        compiler_params=PARAMS,
        cost_estimate=pl.CostEstimate(
            flops=2 * nb * reps * tm * depth * ncols,
            bytes_accessed=2 * (depth * ncols + nb * reps * tm * (depth + ncols)),
            transcendentals=0),
    )(*[b.reshape(1).astype(jnp.int32) for b in blocks], *([attn] * nb), w, *deps)


def add_rows(res, near, far, row0, rows, tr, peers, deps, collective_id):
    cols = res.shape[1]
    nn, nf, per = len(near), len(far), len(far[0])
    widths = [piece.shape[1] for piece in far[0]]
    flat = [piece for group in far for piece in group]
    steps = rows // tr

    def body(*refs):
        r_ref, near_refs, far_refs = refs[0], refs[1:1 + nn], refs[1 + nn:1 + nn + nf * per]
        h_ref, sq_ref, mine, theirs, send_sem, recv_sem = refs[-6:]
        i = pl.program_id(0)
        peer = {"tp2": peers - 1 - lax.axis_index("tp2")}
        barrier = pltpu.get_barrier_semaphore()

        @pl.when(i == 0)
        def _():
            pl.semaphore_signal(barrier, inc=1, device_id=peer, device_id_type=pl.DeviceIdType.MESH)

        total = jnp.zeros((tr, 1), F32)
        base = 0
        for c, width in enumerate(widths):
            sl = slice(base, base + width)
            terms = [ref[:, sl] for ref in near_refs] + [far_refs[g * per + c][...] for g in range(nf)]
            y = terms[0].astype(F32)
            for term in terms[1:]:
                y = y + term.astype(F32)
            h = r_ref[:, sl].astype(F32) + y
            h_ref[:, sl] = h
            total = total + jnp.sum(h * h, axis=-1, keepdims=True)
            base += width
        mine[pl.ds(pl.multiple_of(i * tr, tr), tr), :] = jnp.broadcast_to(total, (tr, 128))

        @pl.when(i == steps - 1)
        def _():
            pl.semaphore_wait(barrier, 1)
            copy = pltpu.make_async_remote_copy(
                src_ref=mine, dst_ref=theirs, send_sem=send_sem, recv_sem=recv_sem,
                device_id=peer, device_id_type=pl.DeviceIdType.MESH)
            copy.start()
            copy.wait()
            sq_ref[...] = mine[...] + theirs[...]

    b0 = row0 // tr if near else 0
    full = pl.BlockSpec((tr, cols), lambda i: (b0 + i, 0))
    in_specs = [full] * (1 + nn) + [pl.BlockSpec((tr, piece.shape[1]), lambda i: (i, 0)) for piece in flat] + [ANY] * len(deps)
    return pl.pallas_call(
        body,
        grid=(steps,),
        in_specs=in_specs,
        out_specs=[pl.BlockSpec((tr, cols), lambda i: (i, 0)), pl.BlockSpec((rows, 128), lambda i: (0, 0))],
        out_shape=[jax.ShapeDtypeStruct((rows, cols), F32), jax.ShapeDtypeStruct((rows, 128), F32)],
        scratch_shapes=[
            pltpu.VMEM((rows, 128), F32),
            pltpu.VMEM((rows, 128), F32),
            pltpu.SemaphoreType.DMA,
            pltpu.SemaphoreType.DMA,
        ],
        compiler_params=pltpu.CompilerParams(vmem_limit_bytes=SMALL_VMEM, collective_id=collective_id, has_side_effects=True),
        cost_estimate=pl.CostEstimate(flops=8 * rows * cols, bytes_accessed=14 * rows * cols, transcendentals=0),
    )(res, *near, *flat, *deps)


def near_sum(res, near, row0, rows, deps):
    cols = res.shape[1]

    def body(*refs):
        total = refs[0][...].astype(F32)
        for ref in refs[1:1 + len(near)]:
            total = total + ref[...].astype(F32)
        refs[-1][...] = total

    return pl.pallas_call(
        body,
        grid=(rows // 16,),
        in_specs=[pl.BlockSpec((16, cols), lambda i: (row0 // 16 + i, 0))] * (1 + len(near)) + [ANY] * len(deps),
        out_specs=pl.BlockSpec((16, cols), lambda i: (i, 0)),
        out_shape=jax.ShapeDtypeStruct((rows, cols), F32),
        compiler_params=pltpu.CompilerParams(vmem_limit_bytes=SMALL_VMEM),
        cost_estimate=pl.CostEstimate(flops=2 * rows * cols, bytes_accessed=10 * rows * cols, transcendentals=0),
    )(res, *near, *deps)


def norm_rows(h, sq, gain, width, total_rows, row0, tr, state):
    rows, cols = h.shape

    def body(*refs):
        h_ref, sq_ref, g_ref, ho_ref, n_ref = refs[0], refs[1], refs[2], refs[-2], refs[-1]
        inv = lax.rsqrt(sq_ref[:, :1] / width + EPS_NORM)
        h = h_ref[...]
        ho_ref[...] = h.astype(BF16)
        n_ref[...] = (h * inv * g_ref[...]).astype(BF16)

    b0 = row0 // tr
    in_specs = [
        pl.BlockSpec((tr, cols), lambda i: (i, 0)),
        pl.BlockSpec((tr, 128), lambda i: (i, 0)),
        pl.BlockSpec((1, cols), lambda i: (0, 0)),
    ] + [ANY] * len(state)
    out = jax.ShapeDtypeStruct((total_rows, cols), BF16)
    return pl.pallas_call(
        body,
        grid=(rows // tr,),
        in_specs=in_specs,
        out_specs=[pl.BlockSpec((tr, cols), lambda i: (b0 + i, 0))] * 2,
        out_shape=[out, out],
        input_output_aliases={3 + i: i for i in range(len(state))},
        compiler_params=pltpu.CompilerParams(vmem_limit_bytes=SMALL_VMEM),
        cost_estimate=pl.CostEstimate(flops=4 * rows * cols, bytes_accessed=8 * rows * cols, transcendentals=0),
    )(h, sq, gain, *state)


def solution(mesh):
    tp = mesh.shape["tp"]
    col_groups = mesh.shape["tp2"]

    def send(x, flip):
        return lax.ppermute(x, "tp", [(i, i ^ flip) for i in range(tp)])

    def inner(attn, w, res, gain):
        me = lax.axis_index("tp")
        rows_total, cols = res.shape
        pieces = {}
        near = None

        got, y = head(attn, w, tp, rows_total, 7)
        pieces[0, HEAD_ROWS] = ([got], [])
        pieces[HEAD_ROWS, HEAD_ROWS] = ([send(y, 2)], [])
        dep = [y]
        for t, (flips, row, tm, splits) in enumerate(PLAN):
            if t == NEAR_AT:
                reps = rows_total // NEAR_ROWS
                other, own = products(attn, w, [(me ^ 1) * reps, me * reps], reps, NEAR_ROWS, 0, cols, 1024, (NEAR_ROWS,), dep)
                dep = [own]
                near = [own, send(other, 1)]
            per = rows_total // tm
            outs = products(attn, w, [(me ^ flip) * per + row // tm for flip in flips], 1, tm, 0, cols, 512, splits, dep)
            dep = [outs[0]]
            for s, size in enumerate(splits):
                into = pieces.setdefault((row, size), ([], []))
                for b, flip in enumerate(flips):
                    into[BOTH.index(flip)].append(send(outs[b * len(splits) + s], flip))
                row += size

        gain2 = gain.reshape(1, cols)
        state = []
        chunks = sorted(pieces)
        for c, (row, size) in enumerate(chunks):
            tr = 32 if (row | size) % 32 == 0 else 16
            if c == 1:
                ready = {k: near_sum(res, near, *chunks[k], state[:1]) for k in range(len(chunks) - 2, len(chunks))}
            terms, step_rows = ((ready[c], []), size) if c >= len(chunks) - 2 else ((res, near), tr)
            h, sq = add_rows(*terms, pieces[row, size], row, size, step_rows, col_groups, state[:1] if state else dep, c)
            state = norm_rows(h, sq, gain2, cols * col_groups, rows_total, row, tr, state)
        return tuple(state)

    row_spec = P(("dp", "tp"), "tp2")
    fn = jax.shard_map(inner, mesh=mesh, in_specs=(P("dp", "tp"), P("tp", "tp2"), row_spec, P("tp2")), out_specs=(row_spec, row_spec), check_vma=False)
    shapes = [jax.ShapeDtypeStruct(s, d) for s, d in (((4096, 16384), BF16), ((16384, 16384), BF16), ((4096, 16384), BF16), ((16384,), F32))]
    jax.eval_shape(fn, *shapes)
    return fn
```
